8 devices in a mesh: dp: 8 (over z, y, x, core).
Axes of the slice: x: 2, y: 2, z: 1, core: 2. Of those that a mesh axis runs over, the one named last changes fastest.
Arguments:
- x_rows: bfloat16 [32768, 896], P('dp')
- dy_rows: bfloat16 [32768, 896], P('dp')
- w_one: bfloat16 [896, 19456], replicated
- w_two: bfloat16 [19456, 896], replicated
- w_three: bfloat16 [896, 4864], replicated
- w_four: bfloat16 [4864, 896], replicated
- master_one: float32 [896, 19456], P('dp')
- master_two: float32 [19456, 896], P('dp')
- master_three: float32 [896, 4864], P('dp')
- master_four: float32 [4864, 896], P('dp')
- m_one: float32 [896, 19456], P('dp')
- m_two: float32 [19456, 896], P('dp')
- m_three: float32 [896, 4864], P('dp')
- m_four: float32 [4864, 896], P('dp')
- v_one: float32 [896, 19456], P('dp')
- v_two: float32 [19456, 896], P('dp')
- v_three: float32 [896, 4864], P('dp')
- v_four: float32 [4864, 896], P('dp')
- learn_rate: float32 [], replicated
- clip_max: float32 [], replicated
Outputs:
- output 1: bfloat16 [896, 19456], replicated
- output 2: bfloat16 [19456, 896], replicated
- output 3: bfloat16 [896, 4864], replicated
- output 4: bfloat16 [4864, 896], replicated
- output 5: float32 [896, 19456], P('dp')
- output 6: float32 [19456, 896], P('dp')
- output 7: float32 [896, 4864], P('dp')
- output 8: float32 [4864, 896], P('dp')
- output 9: float32 [896, 19456], P('dp')
- output 10: float32 [19456, 896], P('dp')
- output 11: float32 [896, 4864], P('dp')
- output 12: float32 [4864, 896], P('dp')
- output 13: float32 [896, 19456], P('dp')
- output 14: float32 [19456, 896], P('dp')
- output 15: float32 [896, 4864], P('dp')
- output 16: float32 [4864, 896], P('dp')
- output 17: float32 [], replicated
All inputs are finite; a program needn't handle non-finite values.
Results may differ from the reference program's by a relative error of at most 0.0111187.
Values are sent between devices in bfloat16 or wider.
A program may use at most 1.25 GiB of HBM per device.

```python
import math
import jax
import jax.numpy as jnp
from jax import lax

MODEL_DIM = 896
FF_DIM = 4864
ROWS_DEV = 4096
DP_SIZE = 8
ADAM_STEP = 10
WIDE_DIM = 4 * FF_DIM
BETA_ONE = 0.9
BETA_TWO = 0.95
ADAM_EPS = 1e-8
NORM_EPS = 1e-6
BIAS_ONE = 1.0 - BETA_ONE ** ADAM_STEP
BIAS_TWO = 1.0 - BETA_TWO ** ADAM_STEP
INV_SQRT2 = 0.7071067811865476
INV_SQRT2PI = 0.3989422804014327
STD_ONE = 1.0 / (1.5 * math.sqrt(MODEL_DIM))
STD_TWO = math.sqrt(2.0 / 0.43) / math.sqrt(WIDE_DIM)
STD_THREE = 1.0 / math.sqrt(2.0 * MODEL_DIM)
STD_FOUR = 1.0 / math.sqrt(0.43 * FF_DIM)


def gelu_value(pre_act):
    pre_wide = pre_act.astype(jnp.float32)
    return 0.5 * pre_wide * (1.0 + lax.erf(pre_wide * INV_SQRT2))


def gelu_slope(pre_act):
    pre_wide = pre_act.astype(jnp.float32)
    return 0.5 * (1.0 + lax.erf(pre_wide * INV_SQRT2)) + pre_wide * INV_SQRT2PI * jnp.exp(-0.5 * pre_wide * pre_wide)


def local_grads(x_rows, dy_rows, w_one, w_two, w_three, w_four):
    z_one = jnp.dot(x_rows, w_one, preferred_element_type=jnp.float32).astype(jnp.bfloat16)
    a_one = gelu_value(z_one).astype(jnp.bfloat16)
    h_two = jnp.dot(a_one, w_two, preferred_element_type=jnp.float32).astype(jnp.bfloat16)
    z_three = jnp.dot(h_two, w_three, preferred_element_type=jnp.float32).astype(jnp.bfloat16)
    a_three = gelu_value(z_three).astype(jnp.bfloat16)
    g_four = jnp.dot(a_three.T, dy_rows, preferred_element_type=jnp.float32)
    da_three = jnp.dot(dy_rows, w_four.T, preferred_element_type=jnp.float32).astype(jnp.bfloat16)
    dz_three = (da_three.astype(jnp.float32) * gelu_slope(z_three)).astype(jnp.bfloat16)
    g_three = jnp.dot(h_two.T, dz_three, preferred_element_type=jnp.float32)
    dh_two = jnp.dot(dz_three, w_three.T, preferred_element_type=jnp.float32).astype(jnp.bfloat16)
    g_two = jnp.dot(a_one.T, dh_two, preferred_element_type=jnp.float32)
    da_one = jnp.dot(dh_two, w_two.T, preferred_element_type=jnp.float32).astype(jnp.bfloat16)
    dz_one = (da_one.astype(jnp.float32) * gelu_slope(z_one)).astype(jnp.bfloat16)
    g_one = jnp.dot(x_rows.T, dz_one, preferred_element_type=jnp.float32)
    return g_one, g_two, g_three, g_four


def mean_grads(x_rows, dy_rows, w_one, w_two, w_three, w_four):
    x_parts = x_rows.reshape(DP_SIZE, ROWS_DEV, MODEL_DIM)
    dy_parts = dy_rows.reshape(DP_SIZE, ROWS_DEV, MODEL_DIM)
    zero_sums = (jnp.zeros((MODEL_DIM, WIDE_DIM), jnp.float32), jnp.zeros((WIDE_DIM, MODEL_DIM), jnp.float32), jnp.zeros((MODEL_DIM, FF_DIM), jnp.float32), jnp.zeros((FF_DIM, MODEL_DIM), jnp.float32))

    def add_part(running, part_pair):
        part_grads = local_grads(part_pair[0], part_pair[1], w_one, w_two, w_three, w_four)
        return tuple(run_sum + new_grad for run_sum, new_grad in zip(running, part_grads)), None

    grad_sums, _unused = lax.scan(add_part, zero_sums, (x_parts, dy_parts))
    return tuple(grad_sum / DP_SIZE for grad_sum in grad_sums)


def adam_rows(grad_mat, master_mat, mom_mat, var_mat, clip_scale, learn_rate):
    scaled = clip_scale * grad_mat
    mom_new = BETA_ONE * mom_mat + (1.0 - BETA_ONE) * scaled
    var_new = BETA_TWO * var_mat + (1.0 - BETA_TWO) * scaled * scaled
    master_new = master_mat - learn_rate * (mom_new / BIAS_ONE) / (jnp.sqrt(var_new / BIAS_TWO) + ADAM_EPS)
    return master_new, mom_new, var_new


def setup_inputs(seed: int = 0) -> dict:
    key_list = jax.random.split(jax.random.key(seed), 16)
    batch_rows = DP_SIZE * ROWS_DEV
    x_rows = (1.5 * jax.random.normal(key_list[0], (batch_rows, MODEL_DIM), jnp.float32)).astype(jnp.bfloat16)
    dy_rows = jax.random.normal(key_list[1], (batch_rows, MODEL_DIM), jnp.float32).astype(jnp.bfloat16)
    shape_list = ((MODEL_DIM, WIDE_DIM), (WIDE_DIM, MODEL_DIM), (MODEL_DIM, FF_DIM), (FF_DIM, MODEL_DIM))
    std_list = (STD_ONE, STD_TWO, STD_THREE, STD_FOUR)
    masters = [std_val * jax.random.normal(key_list[2 + mat_index], shape_list[mat_index], jnp.float32) for mat_index, std_val in enumerate(std_list)]
    weights = [master_mat.astype(jnp.bfloat16) for master_mat in masters]
    grads = mean_grads(x_rows, dy_rows, weights[0], weights[1], weights[2], weights[3])
    grad_norm = jnp.sqrt(sum(jnp.sum(grad_mat * grad_mat) for grad_mat in grads))
    clip_frac = jax.random.uniform(key_list[6], (), jnp.float32, minval=0.3, maxval=0.7)
    clip_max = clip_frac * grad_norm
    learn_rate = jax.random.uniform(key_list[7], (), jnp.float32, minval=0.5, maxval=1.5) / math.sqrt(MODEL_DIM)
    mom_list = []
    var_list = []
    for mat_index, grad_mat in enumerate(grads):
        grad_rms = clip_frac * jnp.sqrt(jnp.mean(grad_mat * grad_mat))
        mom_list.append(0.1 * grad_rms * jax.random.normal(key_list[8 + mat_index], shape_list[mat_index], jnp.float32))
        var_list.append(grad_rms * grad_rms * jax.random.uniform(key_list[12 + mat_index], shape_list[mat_index], jnp.float32, minval=0.5, maxval=1.5))
    return {'x_rows': x_rows, 'dy_rows': dy_rows, 'w_one': weights[0], 'w_two': weights[1], 'w_three': weights[2], 'w_four': weights[3], 'master_one': masters[0], 'master_two': masters[1], 'master_three': masters[2], 'master_four': masters[3], 'm_one': mom_list[0], 'm_two': mom_list[1], 'm_three': mom_list[2], 'm_four': mom_list[3], 'v_one': var_list[0], 'v_two': var_list[1], 'v_three': var_list[2], 'v_four': var_list[3], 'learn_rate': learn_rate, 'clip_max': clip_max}


def reference(x_rows, dy_rows, w_one, w_two, w_three, w_four, master_one, master_two, master_three, master_four, m_one, m_two, m_three, m_four, v_one, v_two, v_three, v_four, learn_rate, clip_max):
    grads = mean_grads(x_rows, dy_rows, w_one, w_two, w_three, w_four)
    grad_norm = jnp.sqrt(sum(jnp.sum(grad_mat * grad_mat) for grad_mat in grads))
    clip_scale = jnp.minimum(1.0, clip_max / (grad_norm + NORM_EPS))
    res_one = adam_rows(grads[0], master_one, m_one, v_one, clip_scale, learn_rate)
    res_two = adam_rows(grads[1], master_two, m_two, v_two, clip_scale, learn_rate)
    res_three = adam_rows(grads[2], master_three, m_three, v_three, clip_scale, learn_rate)
    res_four = adam_rows(grads[3], master_four, m_four, v_four, clip_scale, learn_rate)
    return (res_one[0].astype(jnp.bfloat16), res_two[0].astype(jnp.bfloat16), res_three[0].astype(jnp.bfloat16), res_four[0].astype(jnp.bfloat16), res_one[0], res_two[0], res_three[0], res_four[0], res_one[1], res_two[1], res_three[1], res_four[1], res_one[2], res_two[2], res_three[2], res_four[2], grad_norm)
```

```python
import jax
import jax.numpy as jnp
from jax import lax
from jax.experimental import pallas as pl
from jax.experimental.pallas import tpu as pltpu
from jax.sharding import PartitionSpec as P

ADAM_STEP = 10
BETA_ONE = 0.9
BETA_TWO = 0.95
ADAM_EPS = 1e-8
NORM_EPS = 1e-6
BIAS_ONE = 1.0 - BETA_ONE ** ADAM_STEP
BIAS_TWO = 1.0 - BETA_TWO ** ADAM_STEP
INV_SQRT2 = 0.7071067811865476
INV_SQRT2PI = 0.3989422804014327
F32 = jnp.float32
BF16 = jnp.bfloat16


def adam_rows(grad_mat, master_mat, mom_mat, var_mat, clip_scale, learn_rate):
    scaled = clip_scale * grad_mat
    mom_new = BETA_ONE * mom_mat + (1.0 - BETA_ONE) * scaled
    var_new = BETA_TWO * var_mat + (1.0 - BETA_TWO) * scaled * scaled
    master_new = master_mat - learn_rate * (mom_new / BIAS_ONE) / (jnp.sqrt(var_new / BIAS_TWO) + ADAM_EPS)
    return master_new, mom_new, var_new


def gelu_value(z):
    z = z.astype(F32)
    return (0.5 * z) * (1.0 + lax.erf(z * INV_SQRT2))

def gelu_slope(z):
    z = z.astype(F32)
    return (0.5 + 0.5 * lax.erf(z * INV_SQRT2)) + (z * INV_SQRT2PI) * jnp.exp2(z * (z * (-0.5 * 1.4426950408889634)))

NN = (((1,), (0,)), ((), ()))
NT = (((1,), (1,)), ((), ()))
TN = (((0,), (0,)), ((), ()))
def mm(a, b, dims):
    return lax.dot_general(a, b, dims, preferred_element_type=F32)

def act_call(x, w, rt, nc, name, both):
    rows, k = x.shape
    n = w.shape[1]
    def body(x_ref, w_ref, *outs):
        for j in range(0, n, nc):
            cols = slice(j, min(j + nc, n))
            z = mm(x_ref[...], w_ref[:, cols], NN).astype(BF16)
            if both:
                outs[0][:, cols] = z
            outs[-1][:, cols] = gelu_value(z).astype(BF16)
    ob = pl.BlockSpec((rt, n), lambda i: (i, 0))
    os = jax.ShapeDtypeStruct((rows, n), BF16)
    return pl.pallas_call(body, grid=(rows // rt,),
        in_specs=[pl.BlockSpec((rt, k), lambda i: (i, 0)), pl.BlockSpec((k, n), lambda i: (0, 0))],
        out_specs=[ob] * (2 if both else 1), out_shape=[os] * (2 if both else 1), name=name,
        compiler_params=pltpu.CompilerParams(vmem_limit_bytes=60 << 20),
        cost_estimate=pl.CostEstimate(flops=2 * rows * k * n, bytes_accessed=2 * rows * k + 4 * rows * n, transcendentals=rows * n))(x, w)

def slope_call(d, w, z, rt, nc, name):
    rows, k = d.shape
    n = w.shape[0]
    def body(d_ref, w_ref, z_ref, o_ref):
        for j in range(0, n, nc):
            cols = slice(j, min(j + nc, n))
            da = mm(d_ref[...], w_ref[cols, :], NT).astype(BF16)
            o_ref[:, cols] = (da.astype(F32) * gelu_slope(z_ref[:, cols])).astype(BF16)
    ob = pl.BlockSpec((rt, n), lambda i: (i, 0))
    return pl.pallas_call(body, grid=(rows // rt,),
        in_specs=[pl.BlockSpec((rt, k), lambda i: (i, 0)), pl.BlockSpec((n, k), lambda i: (0, 0)), ob],
        out_specs=ob, out_shape=jax.ShapeDtypeStruct((rows, n), BF16), name=name,
        compiler_params=pltpu.CompilerParams(vmem_limit_bytes=60 << 20),
        cost_estimate=pl.CostEstimate(flops=2 * rows * k * n, bytes_accessed=2 * rows * k + 4 * rows * n, transcendentals=rows * n))(d, w, z)

def tn_call(a, b, kt, nc, name):
    rows, m = a.shape
    n = b.shape[1]
    def body(a_ref, b_ref, o_ref):
        @pl.when(pl.program_id(0) == 0)
        def _():
            o_ref[...] = jnp.zeros_like(o_ref)
        for j in range(0, n, nc):
            cols = slice(j, min(j + nc, n))
            o_ref[:, cols] += mm(a_ref[...], b_ref[:, cols], TN)
    return pl.pallas_call(body, grid=(rows // kt,),
        in_specs=[pl.BlockSpec((kt, m), lambda i: (i, 0)), pl.BlockSpec((kt, n), lambda i: (i, 0))],
        out_specs=pl.BlockSpec((m, n), lambda i: (0, 0)), out_shape=jax.ShapeDtypeStruct((m, n), F32), name=name,
        compiler_params=pltpu.CompilerParams(vmem_limit_bytes=60 << 20),
        cost_estimate=pl.CostEstimate(flops=2 * rows * m * n, bytes_accessed=2 * rows * (m + n), transcendentals=0))(a, b)

def mlp_call(x, w1, w2, rt, wt, sub, name):
    rows, k = x.shape
    n = w1.shape[1]
    steps = n // wt
    def body(x_ref, w1_ref, w2_ref, o_ref, acc_ref):
        @pl.when(pl.program_id(1) == 0)
        def _():
            acc_ref[...] = jnp.zeros_like(acc_ref)
        for r in range(0, rt, sub):
            z = mm(x_ref[r:r + sub, :], w1_ref[...], NN).astype(BF16)
            a = gelu_value(z).astype(BF16)
            acc_ref[r:r + sub, :] += mm(a, w2_ref[...], NN)
        @pl.when(pl.program_id(1) == steps - 1)
        def _():
            o_ref[...] = acc_ref[...].astype(BF16)
    return pl.pallas_call(body, grid=(rows // rt, steps),
        in_specs=[pl.BlockSpec((rt, k), lambda i, j: (i, 0)), pl.BlockSpec((k, wt), lambda i, j: (0, j)), pl.BlockSpec((wt, k), lambda i, j: (j, 0))],
        out_specs=pl.BlockSpec((rt, k), lambda i, j: (i, 0)), out_shape=jax.ShapeDtypeStruct((rows, k), BF16), name=name,
        scratch_shapes=[pltpu.VMEM((rt, k), F32)],
        compiler_params=pltpu.CompilerParams(vmem_limit_bytes=60 << 20),
        cost_estimate=pl.CostEstimate(flops=4 * rows * k * n, bytes_accessed=4 * n * k, transcendentals=rows * n))(x, w1, w2)


def copy_out(mat, steps):
    rows, cols = mat.shape
    block = pl.BlockSpec((rows // steps, cols), lambda i: (i, 0))

    def body(src, dst):
        dst[...] = src[...]

    return pl.pallas_call(
        body, grid=(steps,), in_specs=[block], out_specs=block,
        out_shape=jax.ShapeDtypeStruct(mat.shape, mat.dtype),
        cost_estimate=pl.CostEstimate(flops=10 * rows * cols, bytes_accessed=4 * rows * cols, transcendentals=0),
        name='copy_out')(mat)


def solution(mesh):
    dp = mesh.shape['dp']
    row_spec = P('dp', None)
    rep_spec = P()

    def per_device(x_rows, dy_rows, w_one, w_two, w_three, w_four, master_one, master_two, master_three, master_four, m_one, m_two, m_three, m_four, v_one, v_two, v_three, v_four, learn_rate, clip_max):
        me = lax.axis_index('dp')
        barrier = lax.optimization_barrier
        wide = w_one.shape[1] // dp
        x_all = lax.all_gather(x_rows, 'dp', axis=0, tiled=True)

        h_two = mlp_call(x_rows, w_one, w_two, 1024, 1024, 512, 'mlp_in')
        z_three, a_three = act_call(h_two, w_three, 512, 256, 'act_mid', True)
        dz_three = slope_call(dy_rows, w_four, z_three, 512, 256, 'slope_mid')
        dh_two = mm(dz_three, w_three, NT).astype(BF16)
        dh_two, a_three, dz_late, x_late = barrier((dh_two, a_three, dz_three, x_all))
        dh_all = lax.all_gather(dh_two, 'dp', axis=0, tiled=True)

        w_one_s = lax.dynamic_slice_in_dim(w_one, me * wide, wide, 1)
        w_two_s = lax.dynamic_slice_in_dim(w_two, me * wide, wide, 0)
        g_four = mm(a_three, dy_rows, TN)
        g_three = mm(h_two, dz_late, TN)
        z_sl, a_sl = act_call(x_late, w_one_s, 1024, 256, 'act_slice', True)
        dh_all, g_four, g_three, z_sl, a_sl = barrier((dh_all, g_four, g_three, z_sl, a_sl))
        sh_four = lax.psum_scatter(g_four, 'dp', scatter_dimension=0, tiled=True) / dp
        sh_three = lax.psum_scatter(g_three, 'dp', scatter_dimension=0, tiled=True) / dp

        dz_sl = slope_call(dh_all, w_two_s, z_sl, 512, 256, 'slope_slice')
        g_one_s = tn_call(x_late, dz_sl, 1024, 512, 'grad_one')
        own = g_one_s.shape[0] // dp
        parts = []
        for k in range(dp):
            mine = lax.dynamic_slice_in_dim(g_one_s, (me ^ k) * own, own, 0)
            parts.append(mine if k == 0 else lax.ppermute(mine, 'dp', [(i, i ^ k) for i in range(dp)]))
        a_sl, dh_late, _ = barrier((a_sl, dh_all, g_one_s))
        sh_two = mm(a_sl, dh_late, TN) / dp
        sh_two, *parts = barrier((sh_two, *parts))
        sh_one = jnp.zeros((own, wide * dp), F32)
        for k in range(dp):
            sh_one = lax.dynamic_update_slice_in_dim(sh_one, parts[k], (me ^ k) * wide, 1)
        sh_one = sh_one / dp

        local_sq = sum(jnp.sum(mat * mat) for mat in (g_one_s / dp, sh_two, sh_three, sh_four))
        grad_norm = jnp.sqrt(lax.psum(local_sq, 'dp'))
        clip_scale = jnp.minimum(1.0, clip_max / (grad_norm + NORM_EPS))

        def update(shard, master, mom, var, after):
            if after is not None:
                shard, _ = barrier((shard, after))
            res = adam_rows(shard, master, mom, var, clip_scale, learn_rate)
            return res, res[0].astype(BF16)

        res_four, low_four = update(sh_four, master_four, m_four, v_four, None)
        new_four = lax.all_gather(low_four, 'dp', axis=0, tiled=True)
        res_two, low_two = update(sh_two, master_two, m_two, v_two, low_four)
        new_two = lax.all_gather(low_two, 'dp', axis=0, tiled=True)
        res_one, low_one = update(sh_one, master_one, m_one, v_one, low_two)
        new_four = copy_out(new_four, 4)
        low_one, new_four = barrier((low_one, new_four))
        new_one = lax.all_gather(low_one, 'dp', axis=0, tiled=True)
        res_three, low_three = update(sh_three, master_three, m_three, v_three, low_one)
        low_three, new_two = barrier((low_three, new_two))
        new_three = lax.all_gather(low_three, 'dp', axis=0, tiled=True)
        new_two = copy_out(new_two, 16)
        new_one, new_two = barrier((new_one, new_two))
        new_one = copy_out(new_one, 14)
        new_three, new_one = barrier((new_three, new_one))
        new_three = copy_out(new_three, 7)
        results = (res_one, res_two, res_three, res_four)
        return (new_one, new_two, new_three, new_four) + tuple(r[0] for r in results) + tuple(r[1] for r in results) + tuple(r[2] for r in results) + (grad_norm,)

    in_specs = (row_spec, row_spec) + (rep_spec,) * 4 + (row_spec,) * 12 + (rep_spec, rep_spec)
    out_specs = (rep_spec,) * 4 + (row_spec,) * 12 + (rep_spec,)
    return jax.shard_map(per_device, mesh=mesh, in_specs=in_specs, out_specs=out_specs, check_vma=False)
```

```python
import jax
import jax.numpy as jnp
from jax import lax
from jax.experimental import pallas as pl
from jax.experimental.pallas import tpu as pltpu
from jax.sharding import PartitionSpec as P

ADAM_STEP = 10
BETA_ONE = 0.9
BETA_TWO = 0.95
ADAM_EPS = 1e-8
NORM_EPS = 1e-6
BIAS_ONE = 1.0 - BETA_ONE ** ADAM_STEP
BIAS_TWO = 1.0 - BETA_TWO ** ADAM_STEP
INV_SQRT2 = 0.7071067811865476
INV_SQRT2PI = 0.3989422804014327
F32 = jnp.float32
BF16 = jnp.bfloat16


def adam_rows(grad_mat, master_mat, mom_mat, var_mat, clip_scale, learn_rate):
    scaled = clip_scale * grad_mat
    mom_new = BETA_ONE * mom_mat + (1.0 - BETA_ONE) * scaled
    var_new = BETA_TWO * var_mat + (1.0 - BETA_TWO) * scaled * scaled
    master_new = master_mat - learn_rate * (mom_new / BIAS_ONE) / (jnp.sqrt(var_new / BIAS_TWO) + ADAM_EPS)
    return master_new, mom_new, var_new


def gelu_value(z):
    z = z.astype(F32)
    return (0.5 * z) * (1.0 + lax.erf(z * INV_SQRT2))

def gelu_slope(z):
    z = z.astype(F32)
    return (0.5 + 0.5 * lax.erf(z * INV_SQRT2)) + (z * INV_SQRT2PI) * jnp.exp2(z * (z * (-0.5 * 1.4426950408889634)))

NN = (((1,), (0,)), ((), ()))
NT = (((1,), (1,)), ((), ()))
TN = (((0,), (0,)), ((), ()))
def mm(a, b, dims):
    return lax.dot_general(a, b, dims, preferred_element_type=F32)

def tile_params():
    return pltpu.CompilerParams(vmem_limit_bytes=60 << 20)


def act_call(index, x, w, n, rt, nc, name):
    rows, k = x.shape

    def body(_, x_ref, w_ref, z_ref, a_ref):
        for j in range(0, n, nc):
            cols = slice(j, min(j + nc, n))
            z = mm(x_ref[...], w_ref[:, cols], NN).astype(BF16)
            z_ref[:, cols] = z
            a_ref[:, cols] = gelu_value(z).astype(BF16)

    ob = pl.BlockSpec((rt, n), lambda i, s: (i, 0))
    spec = pltpu.PrefetchScalarGridSpec(
        num_scalar_prefetch=1, grid=(rows // rt,),
        in_specs=[pl.BlockSpec((rt, k), lambda i, s: (i, 0)), pl.BlockSpec((k, n), lambda i, s: (0, s[0]))],
        out_specs=[ob, ob])
    return pl.pallas_call(
        body, grid_spec=spec, out_shape=[jax.ShapeDtypeStruct((rows, n), BF16)] * 2, name=name, compiler_params=tile_params(),
        cost_estimate=pl.CostEstimate(flops=2 * rows * k * n, bytes_accessed=2 * rows * k + 4 * rows * n, transcendentals=rows * n))(index, x, w)


def slope_call(index, d, w, z, rt, nc, name):
    rows, k = d.shape
    n = z.shape[1]

    def body(_, d_ref, w_ref, z_ref, o_ref):
        for j in range(0, n, nc):
            cols = slice(j, min(j + nc, n))
            da = mm(d_ref[...], w_ref[cols, :], NT).astype(BF16)
            o_ref[:, cols] = (da.astype(F32) * gelu_slope(z_ref[:, cols])).astype(BF16)

    ob = pl.BlockSpec((rt, n), lambda i, s: (i, 0))
    spec = pltpu.PrefetchScalarGridSpec(
        num_scalar_prefetch=1, grid=(rows // rt,),
        in_specs=[pl.BlockSpec((rt, k), lambda i, s: (i, 0)), pl.BlockSpec((n, k), lambda i, s: (s[0], 0)), ob],
        out_specs=ob)
    return pl.pallas_call(
        body, grid_spec=spec, out_shape=jax.ShapeDtypeStruct((rows, n), BF16), name=name, compiler_params=tile_params(),
        cost_estimate=pl.CostEstimate(flops=2 * rows * k * n, bytes_accessed=2 * rows * k + 4 * rows * n, transcendentals=rows * n))(index, d, w, z)


def grad_call(index, a, b, kt, nc, scale, pieces, name):
    rows, m = a.shape
    n = b.shape[1]
    steps = rows // kt

    def body(idx_ref, a_ref, b_ref, *refs):
        *outs, sq_ref, acc_ref = refs
        step = pl.program_id(0)

        @pl.when(step == 0)
        def _():
            acc_ref[...] = jnp.zeros_like(acc_ref)

        for j in range(0, n, nc):
            cols = slice(j, min(j + nc, n))
            acc_ref[:, cols] += mm(a_ref[...], b_ref[:, cols], TN)

        @pl.when(step == steps - 1)
        def _():
            total = jnp.zeros((8, 128), F32)
            if pieces:
                own = m // pieces
                for k in range(pieces):
                    start = pl.multiple_of((idx_ref[0] ^ k) * own, 8)
                    for j in range(0, n, 128):
                        val = acc_ref[pl.ds(start, own), j:j + 128] * scale
                        outs[k][:, j:j + 128] = val
                        total = total + jnp.sum((val * val).reshape(own // 8, 8, 128), axis=0)
            else:
                for j in range(0, n, 128):
                    val = acc_ref[:, j:j + 128] * scale
                    outs[0][j:j + 128, :] = val.T
                    total = total + jnp.sum((val * val).reshape(m // 8, 8, 128), axis=0)
            sq_ref[...] = total

    shapes = [(m // pieces, n)] * pieces if pieces else [(n, m)]
    shapes.append((8, 128))
    spec = pltpu.PrefetchScalarGridSpec(
        num_scalar_prefetch=1, grid=(steps,),
        in_specs=[pl.BlockSpec((kt, m), lambda i, s: (i, 0)), pl.BlockSpec((kt, n), lambda i, s: (i, 0))],
        out_specs=[pl.BlockSpec(shape, lambda i, s: (0, 0)) for shape in shapes],
        scratch_shapes=[pltpu.VMEM((m, n), F32)])
    return pl.pallas_call(
        body, grid_spec=spec, out_shape=[jax.ShapeDtypeStruct(shape, F32) for shape in shapes], name=name, compiler_params=tile_params(),
        cost_estimate=pl.CostEstimate(flops=2 * rows * m * n, bytes_accessed=2 * rows * (m + n), transcendentals=0))(index, a, b)


def total_call(tile, dp):
    def body(in_ref, out_ref, held, send_sem, recv_sem):
        me = lax.axis_index('dp')
        gate = pltpu.get_barrier_semaphore()
        for k in range(1, dp):
            pl.semaphore_signal(gate, inc=1, device_id=(lax.rem(me + k, dp),), device_id_type=pl.DeviceIdType.MESH)
        pl.semaphore_wait(gate, dp - 1)
        copies = []
        for k in range(1, dp):
            copies.append(pltpu.make_async_remote_copy(
                src_ref=in_ref, dst_ref=held.at[me], send_sem=send_sem.at[k], recv_sem=recv_sem.at[k],
                device_id=(lax.rem(me + k, dp),), device_id_type=pl.DeviceIdType.MESH))
            copies[-1].start()
        held[me] = in_ref[...]
        for copy in copies:
            copy.wait()
        total = held[0]
        for k in range(1, dp):
            total = total + held[k]
        out_ref[...] = total

    return pl.pallas_call(
        body, out_shape=jax.ShapeDtypeStruct(tile.shape, F32), name='norm_total',
        in_specs=[pl.BlockSpec(memory_space=pltpu.VMEM)], out_specs=pl.BlockSpec(memory_space=pltpu.VMEM),
        scratch_shapes=[pltpu.VMEM((dp,) + tile.shape, F32), pltpu.SemaphoreType.DMA((dp,)), pltpu.SemaphoreType.DMA((dp,))],
        compiler_params=pltpu.CompilerParams(collective_id=0, has_side_effects=True),
        cost_estimate=pl.CostEstimate(flops=1000, bytes_accessed=1 << 16, transcendentals=0))(tile)


def mlp_call(x, w1, w2, rt, wt, sub, name):
    rows, k = x.shape
    n = w1.shape[1]
    steps = n // wt
    def body(x_ref, w1_ref, w2_ref, o_ref, acc_ref):
        @pl.when(pl.program_id(1) == 0)
        def _():
            acc_ref[...] = jnp.zeros_like(acc_ref)
        for r in range(0, rt, sub):
            z = mm(x_ref[r:r + sub, :], w1_ref[...], NN).astype(BF16)
            a = gelu_value(z).astype(BF16)
            acc_ref[r:r + sub, :] += mm(a, w2_ref[...], NN)
        @pl.when(pl.program_id(1) == steps - 1)
        def _():
            o_ref[...] = acc_ref[...].astype(BF16)
    return pl.pallas_call(body, grid=(rows // rt, steps),
        in_specs=[pl.BlockSpec((rt, k), lambda i, j: (i, 0)), pl.BlockSpec((k, wt), lambda i, j: (0, j)), pl.BlockSpec((wt, k), lambda i, j: (j, 0))],
        out_specs=pl.BlockSpec((rt, k), lambda i, j: (i, 0)), out_shape=jax.ShapeDtypeStruct((rows, k), BF16), name=name,
        scratch_shapes=[pltpu.VMEM((rt, k), F32)],
        compiler_params=pltpu.CompilerParams(vmem_limit_bytes=60 << 20),
        cost_estimate=pl.CostEstimate(flops=4 * rows * k * n, bytes_accessed=4 * n * k, transcendentals=rows * n))(x, w1, w2)


def copy_out(mat, steps):
    rows, cols = mat.shape
    block = pl.BlockSpec((rows // steps, cols), lambda i: (i, 0))

    def body(src, dst):
        dst[...] = src[...]

    return pl.pallas_call(
        body, grid=(steps,), in_specs=[block], out_specs=block,
        out_shape=jax.ShapeDtypeStruct(mat.shape, mat.dtype),
        cost_estimate=pl.CostEstimate(flops=10 * rows * cols, bytes_accessed=4 * rows * cols, transcendentals=0),
        name='copy_out')(mat)


def solution(mesh):
    dp = mesh.shape['dp']
    row_spec = P('dp', None)
    rep_spec = P()

    def per_device(x_rows, dy_rows, w_one, w_two, w_three, w_four, master_one, master_two, master_three, master_four, m_one, m_two, m_three, m_four, v_one, v_two, v_three, v_four, learn_rate, clip_max):
        me = lax.axis_index('dp')
        barrier = lax.optimization_barrier
        wide = w_one.shape[1] // dp
        x_all = lax.all_gather(x_rows, 'dp', axis=0, tiled=True)

        h_two = mlp_call(x_rows, w_one, w_two, 1024, 1024, 512, 'mlp_in')
        first = jnp.zeros((1,), jnp.int32)
        mine = jnp.full((1,), me, jnp.int32)
        z_three, a_three = act_call(first, h_two, w_three, w_three.shape[1], 512, 256, 'act_mid')
        dz_three = slope_call(first, dy_rows, w_four, z_three, 512, 256, 'slope_mid')
        dh_two = mm(dz_three, w_three, NT).astype(BF16)
        dh_two, a_three, dz_late, x_late = barrier((dh_two, a_three, dz_three, x_all))
        dh_all = lax.all_gather(dh_two, 'dp', axis=0, tiled=True)

        g_four = mm(a_three, dy_rows, TN)
        g_three = mm(h_two, dz_late, TN)
        z_sl, a_sl = act_call(mine, x_late, w_one, wide, 1024, 256, 'act_slice')
        dh_all, g_four, g_three, z_sl, a_sl = barrier((dh_all, g_four, g_three, z_sl, a_sl))
        sh_four = lax.psum_scatter(g_four, 'dp', scatter_dimension=0, tiled=True) / dp
        sh_three = lax.psum_scatter(g_three, 'dp', scatter_dimension=0, tiled=True) / dp

        dz_sl = slope_call(mine, dh_all, w_two, z_sl, 512, 256, 'slope_slice')
        *blocks, sq_one = grad_call(mine, x_late, dz_sl, 1024, 512, 1.0 / dp, dp, 'grad_one')
        parts = [blocks[0]] + [lax.ppermute(blocks[k], 'dp', [(i, i ^ k) for i in range(dp)]) for k in range(1, dp)]
        sq_small = jnp.sum(sh_three * sh_three) + jnp.sum(sh_four * sh_four)
        a_sl, dh_late, sq_small, sq_one = barrier((a_sl, dh_all, sq_small, sq_one))
        sh_two, sq_two = grad_call(mine, dh_late, a_sl, 1024, 512, 1.0 / dp, 0, 'grad_two')
        sh_two, sq_two, *parts = barrier((sh_two, sq_two, *parts))
        sh_one = jnp.zeros((blocks[0].shape[0], wide * dp), F32)
        for k in range(dp):
            sh_one = lax.dynamic_update_slice_in_dim(sh_one, parts[k], (me ^ k) * wide, 1)

        local_sq = jnp.sum(sq_one + sq_two) + sq_small
        grad_norm = jnp.sqrt(total_call(jnp.full((8, 128), local_sq, F32), dp)[0, 0])
        clip_scale = jnp.minimum(1.0, clip_max / (grad_norm + NORM_EPS))

        def update(shard, master, mom, var, after):
            if after is not None:
                shard, _ = barrier((shard, after))
            res = adam_rows(shard, master, mom, var, clip_scale, learn_rate)
            return res, res[0].astype(BF16)

        res_four, low_four = update(sh_four, master_four, m_four, v_four, None)
        new_four = lax.all_gather(low_four, 'dp', axis=0, tiled=True)
        res_two, low_two = update(sh_two, master_two, m_two, v_two, low_four)
        new_two = lax.all_gather(low_two, 'dp', axis=0, tiled=True)
        res_one, low_one = update(sh_one, master_one, m_one, v_one, low_two)
        new_four = copy_out(new_four, 4)
        low_one, new_four = barrier((low_one, new_four))
        new_one = lax.all_gather(low_one, 'dp', axis=0, tiled=True)
        res_three, low_three = update(sh_three, master_three, m_three, v_three, low_one)
        low_three, new_two = barrier((low_three, new_two))
        new_three = lax.all_gather(low_three, 'dp', axis=0, tiled=True)
        new_two = copy_out(new_two, 16)
        new_one, new_two = barrier((new_one, new_two))
        new_one = copy_out(new_one, 14)
        new_three, new_one = barrier((new_three, new_one))
        new_three = copy_out(new_three, 7)
        results = (res_one, res_two, res_three, res_four)
        return (new_one, new_two, new_three, new_four) + tuple(r[0] for r in results) + tuple(r[1] for r in results) + tuple(r[2] for r in results) + (grad_norm,)

    in_specs = (row_spec, row_spec) + (rep_spec,) * 4 + (row_spec,) * 12 + (rep_spec, rep_spec)
    out_specs = (rep_spec,) * 4 + (row_spec,) * 12 + (rep_spec,)
    return jax.shard_map(per_device, mesh=mesh, in_specs=in_specs, out_specs=out_specs, check_vma=False)
```
